32 devices in a mesh: space: 8 (over y, x, core), sect: 4 (over z).
Axes of the slice: x: 2, y: 2, z: 4, core: 2. Of those that a mesh axis runs over, the one named last changes fastest.
Arguments:
- density: float32 [24, 128, 2048], P('space', 'sect'), may hold values from 0.05 to 1
- velocity: float32 [24, 2048], P('space'), may hold values from -0.9 to 0.9
- kernel: float32 [128, 128], replicated, may hold values from 0.00078125 to 0.0078125
- split: float32 [128, 128], replicated, may hold values from 0 to 1
- target: int32 [128, 128], replicated, may hold values from 0 to 126, as said below
Outputs:
- updated: float32 [24, 128, 2048], P('space', 'sect')
The draws below stay inside these ranges and needn't reach their ends.
Inputs may be any that keep to these rules, and one draw needn't show every extreme that they name: target is symmetric, and target[i][j] is at least min(max(i, j), 126).
All inputs are finite; a program needn't handle non-finite values.
Results may differ from the reference program's by a relative error of at most 0.00058.
Values may be sent and summed in bfloat16 or wider, within the bound.
A program may use at most 64 MiB of HBM per device.

```python
import math
import jax
import jax.numpy as jnp
from jax import lax

K = 128
STEPS = 4
PL = 2048
NX = 24


def draw_target(key, part):
    rows = lax.broadcasted_iota(jnp.int32, (K, K), 0)
    cols = lax.broadcasted_iota(jnp.int32, (K, K), 1)
    lowest = jnp.minimum(jnp.maximum(rows, cols), K - 2)
    spread = K - 1 - lowest
    raw = jax.random.randint(key, (K, K), 0, 1048576)
    raw = jnp.where(rows <= cols, raw, raw.T)
    return (lowest + raw % spread).astype(jnp.int32)


def block_levels(stream_key, extent, cuts, low, high):
    factor_of, own = 1.0, jax.random.fold_in(stream_key, 6)
    for position, shards_of in cuts:
        heights = jnp.exp(jax.random.uniform(jax.random.fold_in(own, position), (shards_of,), jnp.float32, low / len(cuts), high / len(cuts)))
        factor_of = factor_of * jnp.repeat(heights, extent[position] // shards_of).reshape([-1 if axis == position else 1 for axis in range(len(extent))])
    return factor_of


def setup_inputs(seed: int = 0) -> dict:
    streams_of = jax.random.split(jax.random.key(seed), 6)
    density = jnp.clip(jnp.exp(math.log(1.0) - 2.9957323 * jax.random.uniform(streams_of[0], (NX, K, PL), jnp.float32) ** block_levels(streams_of[0], (NX, K, PL), ((0, 8), (1, 4)), -0.2, 0.2)), 0.05, 1.0)
    velocity = jnp.clip(jax.random.uniform(streams_of[1], (NX, PL), jnp.float32, -0.9, 0.9) * block_levels(streams_of[1], (NX, PL), ((0, 8),), -0.4, 0.0), -0.9, 0.9)
    kernel = jnp.clip(jnp.exp(jax.random.uniform(streams_of[2], (K, K), jnp.float32, math.log(0.00078125), math.log(0.0078125))), 0.00078125, 0.0078125)
    split = jnp.clip(jax.random.uniform(streams_of[3], (K, K), jnp.float32, 0.0, 1.0), 0.0, 1.0)
    target = draw_target(jax.random.fold_in(streams_of[5], 71), 0)
    return {"density": density, "velocity": velocity, "kernel": kernel, "split": split, "target": target}


def reference(density, velocity, kernel, split, target):
    beta = 0.5 * (kernel + kernel.T)
    weight = 0.5 * (split + split.T)
    beta_low = beta.astype(jnp.bfloat16)
    ks = jnp.arange(K, dtype=jnp.int32)[:, None, None]
    tt = target[None, :, :]
    coef = (0.5 * beta[None] * (weight[None] * (ks == tt).astype(jnp.float32) + (1.0 - weight[None]) * (ks == tt + 1).astype(jnp.float32))).astype(jnp.bfloat16).reshape(K, K * K)
    coef_wide = coef.astype(jnp.float32)

    def plane(row):
        wide = row.astype(jnp.float32)
        pair = (wide[:, None, :] * wide[None, :, :]).astype(jnp.bfloat16).reshape(K * K, row.shape[-1])
        gain = jnp.dot(coef_wide, pair.astype(jnp.float32), precision=lax.Precision.HIGHEST)
        rate = jnp.dot(beta_low, row, preferred_element_type=jnp.float32)
        return gain, rate

    speed = velocity[:, None, :]
    state = density
    for step in range(STEPS):
        low = state.astype(jnp.bfloat16)
        gain, rate = lax.map(plane, low)
        ahead = jnp.roll(state, -1, axis=0)
        flux = jnp.maximum(speed, 0.0) * state + jnp.minimum(speed, 0.0) * ahead
        behind = jnp.roll(flux, 1, axis=0)
        state = state - (flux - behind) + (gain - state * rate)
    return state
```

```python
import jax
import jax.numpy as jnp
from jax import lax
from jax.experimental import pallas as pl
from jax.experimental.pallas import tpu as pltpu
from jax.sharding import PartitionSpec as P

STEPS = 4
LANES = 128
ROWS = 16
DEEP = 256


def unit_list(sections):
    blocks = sections // ROWS
    units = [(0, i, None) for i in range(ROWS)]
    for b in range(1, blocks // 2):
        units += [(b, ROWS * b + r, ROWS * (blocks - b) + r) for r in range(ROWS)]
    half = blocks // 2
    units += [(half, ROWS * half + r, ROWS * half + ROWS // 2 + r) for r in range(ROWS // 2)]
    return units


def fold_tables(table, share, sections):
    blocks = sections // ROWS
    lane = lax.broadcasted_iota(jnp.int32, (ROWS, sections), 1)
    pieces = [table[:ROWS]]
    for b in range(1, blocks // 2):
        near = table[ROWS * b : ROWS * (b + 1)]
        far = table[ROWS * (blocks - b) : ROWS * (blocks - b + 1)]
        pieces.append(jnp.where(lane < ROWS * b, pltpu.roll(far, ROWS * b, 1), near))
    half = blocks // 2
    near = table[ROWS * half : ROWS * half + ROWS // 2]
    far = table[ROWS * half + ROWS // 2 : ROWS * (half + 1)]
    pieces.append(
        jnp.where(lane[: ROWS // 2] < ROWS * half, pltpu.roll(far, ROWS * half, 1), near)
    )
    return jnp.concatenate(pieces, axis=0)


def build_coefficients(kernel_ref, split_ref, target_ref, tt, bb, ww, coef):
    sections = kernel_ref.shape[0]
    beta = 0.5 * (kernel_ref[...] + kernel_ref[...].T)
    weight = 0.5 * (split_ref[...] + split_ref[...].T)
    row = lax.broadcasted_iota(jnp.int32, (sections, sections), 0)
    col = lax.broadcasted_iota(jnp.int32, (sections, sections), 1)
    share = jnp.where(col > row, 1.0, jnp.where(col == row, 0.5, 0.0)) * beta
    tt[...] = fold_tables(target_ref[...], None, sections)
    bb[...] = fold_tables(share, None, sections)
    ww[...] = fold_tables(weight, None, sections)
    ks = lax.broadcasted_iota(jnp.int32, (sections, sections), 0)

    def one(tile, carry):
        for part in range(DEEP // sections):
            unit = tile * (DEEP // sections) + part
            t = tt[pl.ds(unit, 1), :]
            b = bb[pl.ds(unit, 1), :]
            w = ww[pl.ds(unit, 1), :]
            low = b * w
            high = b * (1.0 - w)
            value = jnp.where(ks == t, low, jnp.where(ks == t + 1, high, 0.0))
            coef[tile, :, part * sections : (part + 1) * sections] = value.astype(jnp.bfloat16)
        return carry

    lax.fori_loop(0, coef.shape[0] - 1, one, 0)
    coef[coef.shape[0] - 1] = jnp.concatenate(
        [beta.astype(jnp.bfloat16), jnp.zeros((sections, sections), jnp.bfloat16)], axis=1
    )


def pair_tile(wide, low, tile, units, sections):
    blocks = []
    for part in range(DEEP // sections):
        b, near, far = units[tile * (DEEP // sections) + part]
        if far is not None:
            lead = jnp.broadcast_to(wide[far : far + 1, :], (ROWS, wide.shape[1])).astype(jnp.bfloat16)
            for start in range(sections - ROWS * b, sections, ROWS):
                blocks.append(lead * low[start : start + ROWS, :])
        lead = jnp.broadcast_to(wide[near : near + 1, :], (ROWS, wide.shape[1])).astype(jnp.bfloat16)
        for start in range(ROWS * b, sections, ROWS):
            blocks.append(lead * low[start : start + ROWS, :])
    return jnp.concatenate(blocks, axis=0)


def advance_all(state, speed, coef, tiles, shift):
    sections = state.shape[1]
    units = unit_list(sections)
    count = len(units) * sections // DEEP
    chunk = 2 * LANES if tiles % 2 == 0 else LANES
    engines = 2 if (tiles * LANES // chunk) % 2 == 0 else 1
    trips = tiles * LANES // (chunk * engines)

    def pads(slot):
        state[slot, :, :LANES] = pltpu.roll(
            state[slot, :, tiles * LANES : (tiles + 1) * LANES], shift % LANES, 1
        )
        state[slot, :, (tiles + 1) * LANES :] = pltpu.roll(
            state[slot, :, LANES : 2 * LANES], (LANES - shift) % LANES, 1
        )

    def finish(now, at, gain, rate):
        here = pl.ds(pl.multiple_of(at + LANES, LANES), chunk)
        before = pl.ds(pl.multiple_of(at, LANES), chunk)
        after = pl.ds(pl.multiple_of(at + 2 * LANES, LANES), chunk)
        s = state[now, :, here]
        v, u = speed[:, here], speed[:, before]
        flux = jnp.maximum(v, 0.0) * s + jnp.minimum(v, 0.0) * state[now, :, after]
        behind = jnp.maximum(u, 0.0) * state[now, :, before] + jnp.minimum(u, 0.0) * s
        state[1 - now, :, here] = s - (flux - behind) + (gain - s * rate)

    def step(index, carry):
        now = lax.rem(index, 2)
        pads(now)

        def trip(n, carry):
            def body():
                starts = [(n * engines + q) * chunk for q in range(engines)]
                wides, lows = [], []
                for q in range(engines):
                    here = pl.ds(pl.multiple_of(starts[q] + LANES, LANES), chunk)
                    wide = state.at[now, :, here]
                    wides.append(wide)
                    lows.append(wide[...].astype(jnp.bfloat16))
                for tile in range(count):
                    for q in range(engines):
                        rhs = pair_tile(wides[q], lows[q], tile, units, sections)
                        pltpu.matmul_push_rhs(rhs, staging_register=tile % 2, mxu_index=q)
                        pltpu.matmul_acc_lhs(accs[2 * q], coef[tile], load_staged_rhs=tile % 2)
                for q in range(engines):
                    rhs = jnp.concatenate([lows[q]] * (DEEP // sections), axis=0)
                    pltpu.matmul_push_rhs(rhs, staging_register=count % 2, mxu_index=q)
                    pltpu.matmul_acc_lhs(accs[2 * q + 1], coef[count], load_staged_rhs=count % 2)
                for q in range(engines):
                    gain = pltpu.matmul_pop(accs[2 * q])
                    rate = pltpu.matmul_pop(accs[2 * q + 1])
                    finish(now, starts[q], gain, rate)

            def body_dot():
                start = n * chunk
                here = pl.ds(pl.multiple_of(start + LANES, LANES), chunk)
                wide = state.at[now, :, here]
                low = wide[...].astype(jnp.bfloat16)
                gain = jnp.zeros((sections, chunk), jnp.float32)
                for tile in range(count):
                    rhs = pair_tile(wide, low, tile, units, sections)
                    gain += jnp.dot(coef[tile], rhs, preferred_element_type=jnp.float32)
                rate = jnp.dot(
                    coef[count][:, :sections], low, preferred_element_type=jnp.float32
                )
                finish(now, start, gain, rate)

            if chunk == DEEP:
                body()
            else:
                body_dot()
            return carry

        lax.fori_loop(0, trips, trip, 0)
        return carry

    def every(*found):
        accs.extend(found)
        for acc in found:
            pltpu.matmul_pop(acc)
        lax.fori_loop(0, STEPS, step, 0)

    accs = []
    if chunk == DEEP:
        pl.run_scoped(
            every,
            *[
                pltpu.ACC(q)((sections, DEEP), jnp.float32)
                for q in range(engines)
                for _ in range(2)
            ],
        )
    else:
        every()


def compute_kernel(shift, x_ref, v_ref, kernel_ref, split_ref, target_ref, o_ref, state, speed, tt, bb, ww, coef):
    tiles = x_ref.shape[1] // LANES
    build_coefficients(kernel_ref, split_ref, target_ref, tt, bb, ww, coef)
    width = tiles * LANES
    state[0, :, LANES : LANES + width] = x_ref[...]
    speed[:, LANES : LANES + width] = v_ref[...]
    speed[:, :LANES] = pltpu.roll(v_ref[:, width - LANES :], shift % LANES, 1)
    speed[:, LANES + width :] = pltpu.roll(v_ref[:, :LANES], (LANES - shift) % LANES, 1)
    advance_all(state, speed, coef, tiles, shift)
    o_ref[...] = state[STEPS % 2, :, LANES : LANES + width]


def compute(x, v, kernel, split, target, shift):
    sections, width = x.shape
    units = len(unit_list(sections))
    vmem = pl.BlockSpec(memory_space=pltpu.VMEM)

    def call(*refs):
        compute_kernel(shift, *refs)

    return pl.pallas_call(
        call,
        out_shape=jax.ShapeDtypeStruct((sections, width), jnp.float32),
        in_specs=[vmem] * 5,
        out_specs=vmem,
        scratch_shapes=[
            pltpu.VMEM((2, sections, width + 2 * LANES), jnp.float32),
            pltpu.VMEM((1, width + 2 * LANES), jnp.float32),
            pltpu.VMEM((units, sections), jnp.int32),
            pltpu.VMEM((units, sections), jnp.float32),
            pltpu.VMEM((units, sections), jnp.float32),
            pltpu.VMEM((units * sections // DEEP + 1, sections, DEEP), jnp.bfloat16),
        ],
        name="coagulate",
    )(x, v, kernel, split, target)


def on_device(density, velocity, kernel, split, target):
    planes, block, width = density.shape
    sections = kernel.shape[0]
    space, sect = lax.axis_size("space"), lax.axis_size("sect")
    everyone = space * sect
    share = width // everyone
    groups = LANES // share
    tiles = planes * space // groups
    axes = ("space", "sect")

    sent = density.reshape(planes, block, everyone, share).transpose(2, 0, 1, 3)
    got = lax.all_to_all(sent, axes, 0, 0, tiled=True)
    got = got.reshape(space, sect, planes, block, share).transpose(1, 3, 0, 2, 4)
    got = got.reshape(sections, groups, tiles, share).transpose(0, 2, 1, 3)
    x = got.reshape(sections, tiles * LANES)

    vsent = velocity.reshape(planes, space, width // space).transpose(1, 0, 2)
    vgot = lax.all_to_all(vsent, "space", 0, 0, tiled=True).reshape(planes * space, width // space)
    v = lax.dynamic_slice_in_dim(vgot, lax.axis_index("sect") * share, share, 1)
    v = v.reshape(groups, tiles, share).transpose(1, 0, 2).reshape(1, tiles * LANES)

    y = compute(x, v, kernel, split, target, share)

    y = y.reshape(sections, tiles, groups, share).transpose(0, 2, 1, 3)
    y = y.reshape(sect, block, space, planes, share).transpose(2, 0, 3, 1, 4)
    y = y.reshape(everyone, planes, block, share)
    back = lax.all_to_all(y, axes, 0, 0, tiled=True)
    return back.transpose(1, 2, 0, 3).reshape(planes, block, width)


def solution(mesh):
    def run(*arrays):
        placed = (P("space", "sect", None), P("space", None), P(), P(), P())
        return jax.shard_map(
            on_device, mesh=mesh, in_specs=placed, out_specs=P("space", "sect", None), check_vma=False
        )(*arrays)

    def traced(*arrays):
        with jax.sharding.use_abstract_mesh(mesh.abstract_mesh):
            return run(*arrays)

    return traced
```

```python
import jax
import jax.numpy as jnp
from jax import lax
from jax.experimental import pallas as pl
from jax.experimental.pallas import tpu as pltpu
from jax.sharding import PartitionSpec as P

STEPS = 4
LANES = 128
ROWS = 16
DEEP = 256


def unit_list(sections):
    blocks = sections // ROWS
    units = [(0, i, None) for i in range(ROWS)]
    for b in range(1, blocks // 2):
        units += [(b, ROWS * b + r, ROWS * (blocks - b) + r) for r in range(ROWS)]
    half = blocks // 2
    units += [(half, ROWS * half + r, ROWS * half + ROWS // 2 + r) for r in range(ROWS // 2)]
    return units


def fold_tables(table, share, sections):
    blocks = sections // ROWS
    lane = lax.broadcasted_iota(jnp.int32, (ROWS, sections), 1)
    pieces = [table[:ROWS]]
    for b in range(1, blocks // 2):
        near = table[ROWS * b : ROWS * (b + 1)]
        far = table[ROWS * (blocks - b) : ROWS * (blocks - b + 1)]
        pieces.append(jnp.where(lane < ROWS * b, pltpu.roll(far, ROWS * b, 1), near))
    half = blocks // 2
    near = table[ROWS * half : ROWS * half + ROWS // 2]
    far = table[ROWS * half + ROWS // 2 : ROWS * (half + 1)]
    pieces.append(
        jnp.where(lane[: ROWS // 2] < ROWS * half, pltpu.roll(far, ROWS * half, 1), near)
    )
    return jnp.concatenate(pieces, axis=0)


def build_coefficients(kernel_ref, split_ref, target_ref, tt, bb, ww, coef):
    sections = kernel_ref.shape[0]
    beta = 0.5 * (kernel_ref[...] + kernel_ref[...].T)
    weight = 0.5 * (split_ref[...] + split_ref[...].T)
    row = lax.broadcasted_iota(jnp.int32, (sections, sections), 0)
    col = lax.broadcasted_iota(jnp.int32, (sections, sections), 1)
    share = jnp.where(col > row, 1.0, jnp.where(col == row, 0.5, 0.0)) * beta
    tt[...] = fold_tables(target_ref[...], None, sections)
    bb[...] = fold_tables(share, None, sections)
    ww[...] = fold_tables(weight, None, sections)
    ks = lax.broadcasted_iota(jnp.int32, (sections, sections), 0)

    def one(tile, carry):
        for part in range(DEEP // sections):
            unit = tile * (DEEP // sections) + part
            t = tt[pl.ds(unit, 1), :]
            b = bb[pl.ds(unit, 1), :]
            w = ww[pl.ds(unit, 1), :]
            low = b * w
            high = b * (1.0 - w)
            value = jnp.where(ks == t, low, jnp.where(ks == t + 1, high, 0.0))
            coef[tile, :, part * sections : (part + 1) * sections] = value.astype(jnp.bfloat16)
        return carry

    lax.fori_loop(0, coef.shape[0] - 1, one, 0)
    coef[coef.shape[0] - 1] = jnp.concatenate(
        [beta.astype(jnp.bfloat16), jnp.zeros((sections, sections), jnp.bfloat16)], axis=1
    )


def pair_tile(wide, low, tile, units, sections):
    blocks = []
    for part in range(DEEP // sections):
        b, near, far = units[tile * (DEEP // sections) + part]
        if far is not None:
            lead = jnp.broadcast_to(wide[far : far + 1, :], (ROWS, wide.shape[1])).astype(jnp.bfloat16)
            for start in range(sections - ROWS * b, sections, ROWS):
                blocks.append(lead * low[start : start + ROWS, :])
        lead = jnp.broadcast_to(wide[near : near + 1, :], (ROWS, wide.shape[1])).astype(jnp.bfloat16)
        for start in range(ROWS * b, sections, ROWS):
            blocks.append(lead * low[start : start + ROWS, :])
    return jnp.concatenate(blocks, axis=0)


def advance_all(state, speed, coef, tiles, shift):
    sections = state.shape[1]
    units = unit_list(sections)
    count = len(units) * sections // DEEP
    chunk = 2 * LANES if tiles % 2 == 0 else LANES
    engines = 2 if (tiles * LANES // chunk) % 2 == 0 else 1
    trips = tiles * LANES // (chunk * engines)

    def pads(slot):
        state[slot, :, :LANES] = pltpu.roll(
            state[slot, :, tiles * LANES : (tiles + 1) * LANES], shift % LANES, 1
        )
        state[slot, :, (tiles + 1) * LANES :] = pltpu.roll(
            state[slot, :, LANES : 2 * LANES], (LANES - shift) % LANES, 1
        )

    def finish(now, at, gain, rate):
        here = pl.ds(pl.multiple_of(at + LANES, LANES), chunk)
        before = pl.ds(pl.multiple_of(at, LANES), chunk)
        after = pl.ds(pl.multiple_of(at + 2 * LANES, LANES), chunk)
        s = state[now, :, here]
        v, u = speed[:, here], speed[:, before]
        flux = jnp.maximum(v, 0.0) * s + jnp.minimum(v, 0.0) * state[now, :, after]
        behind = jnp.maximum(u, 0.0) * state[now, :, before] + jnp.minimum(u, 0.0) * s
        state[1 - now, :, here] = s - (flux - behind) + (gain - s * rate)

    def step(index, carry):
        now = lax.rem(index, 2)
        pads(now)

        def trip(n, carry):
            def body():
                starts = [(n * engines + q) * chunk for q in range(engines)]
                wides, lows = [], []
                for q in range(engines):
                    here = pl.ds(pl.multiple_of(starts[q] + LANES, LANES), chunk)
                    wide = state.at[now, :, here]
                    wides.append(wide)
                    lows.append(wide[...].astype(jnp.bfloat16))
                for tile in range(count):
                    for q in range(engines):
                        rhs = pair_tile(wides[q], lows[q], tile, units, sections)
                        pltpu.matmul_push_rhs(rhs, staging_register=tile % 2, mxu_index=q)
                        pltpu.matmul_acc_lhs(accs[2 * q], coef[tile], load_staged_rhs=tile % 2)
                for q in range(engines):
                    rhs = jnp.concatenate([lows[q]] * (DEEP // sections), axis=0)
                    pltpu.matmul_push_rhs(rhs, staging_register=count % 2, mxu_index=q)
                    pltpu.matmul_acc_lhs(accs[2 * q + 1], coef[count], load_staged_rhs=count % 2)
                for q in range(engines):
                    gain = pltpu.matmul_pop(accs[2 * q])
                    rate = pltpu.matmul_pop(accs[2 * q + 1])
                    finish(now, starts[q], gain, rate)

            def body_dot():
                start = n * chunk
                here = pl.ds(pl.multiple_of(start + LANES, LANES), chunk)
                wide = state.at[now, :, here]
                low = wide[...].astype(jnp.bfloat16)
                gain = jnp.zeros((sections, chunk), jnp.float32)
                for tile in range(count):
                    rhs = pair_tile(wide, low, tile, units, sections)
                    gain += jnp.dot(coef[tile], rhs, preferred_element_type=jnp.float32)
                rate = jnp.dot(
                    coef[count][:, :sections], low, preferred_element_type=jnp.float32
                )
                finish(now, start, gain, rate)

            if chunk == DEEP:
                body()
            else:
                body_dot()
            return carry

        lax.fori_loop(0, trips, trip, 0)
        return carry

    def every(*found):
        accs.extend(found)
        for acc in found:
            pltpu.matmul_pop(acc)
        lax.fori_loop(0, STEPS, step, 0)

    accs = []
    if chunk == DEEP:
        pl.run_scoped(
            every,
            *[
                pltpu.ACC(q)((sections, DEEP), jnp.float32)
                for q in range(engines)
                for _ in range(2)
            ],
        )
    else:
        every()


def compute_kernel(shift, x_ref, v_ref, kernel_ref, split_ref, target_ref, o_ref, state, speed, tt, bb, ww, coef):
    tiles = x_ref.shape[1] // LANES
    build_coefficients(kernel_ref, split_ref, target_ref, tt, bb, ww, coef)
    width = tiles * LANES
    state[0, :, LANES : LANES + width] = x_ref[...]
    speed[:, LANES : LANES + width] = v_ref[...]
    speed[:, :LANES] = pltpu.roll(v_ref[:, width - LANES :], shift % LANES, 1)
    speed[:, LANES + width :] = pltpu.roll(v_ref[:, :LANES], (LANES - shift) % LANES, 1)
    advance_all(state, speed, coef, tiles, shift)
    o_ref[...] = state[STEPS % 2, :, LANES : LANES + width]


def compute(x, v, kernel, split, target, shift):
    sections, width = x.shape
    units = len(unit_list(sections))
    vmem = pl.BlockSpec(memory_space=pltpu.VMEM)

    def call(*refs):
        compute_kernel(shift, *refs)

    return pl.pallas_call(
        call,
        out_shape=jax.ShapeDtypeStruct((sections, width), jnp.float32),
        in_specs=[vmem] * 5,
        out_specs=vmem,
        scratch_shapes=[
            pltpu.VMEM((2, sections, width + 2 * LANES), jnp.float32),
            pltpu.VMEM((1, width + 2 * LANES), jnp.float32),
            pltpu.VMEM((units, sections), jnp.int32),
            pltpu.VMEM((units, sections), jnp.float32),
            pltpu.VMEM((units, sections), jnp.float32),
            pltpu.VMEM((units * sections // DEEP + 1, sections, DEEP), jnp.bfloat16),
        ],
        name="coagulate",
    )(x, v, kernel, split, target)


def swap_halves(first, second):
    half = LANES // 2
    left = lax.broadcasted_iota(jnp.int32, first.shape, 1) < half
    return (
        jnp.where(left, first, pltpu.roll(second, half, 1)),
        jnp.where(left, pltpu.roll(first, half, 1), second),
    )


def peer_of(index, sect):
    return {"space": index // sect, "sect": lax.rem(index, sect)}


def greet(me, everyone, sect):
    barrier = pltpu.get_barrier_semaphore()

    def one(k, carry):
        pl.semaphore_signal(
            barrier,
            inc=1,
            device_id=peer_of(lax.rem(me + k, everyone), sect),
            device_id_type=pl.DeviceIdType.MESH,
        )
        return carry

    lax.fori_loop(1, everyone, one, 0)
    return barrier


def message(send, recv, ssem, rsem, me, peer, sect):
    return pltpu.make_async_remote_copy(
        src_ref=send.at[peer],
        dst_ref=recv.at[me],
        send_sem=ssem.at[peer],
        recv_sem=rsem.at[me],
        device_id=peer_of(peer, sect),
        device_id_type=pl.DeviceIdType.MESH,
    )


def send_all(send, recv, ssem, rsem, me, everyone, sect):
    def one(k, carry):
        message(send, recv, ssem, rsem, me, lax.rem(me + k, everyone), sect).start()
        return carry

    lax.fori_loop(1, everyone, one, 0)
    recv[me] = send[me]


def wait_all(send, recv, ssem, rsem, me, everyone, sect):
    def one(k, carry):
        source = lax.rem(me + everyone - k, everyone)
        pltpu.make_async_remote_copy(
            src_ref=send.at[source],
            dst_ref=recv.at[source],
            send_sem=ssem.at[source],
            recv_sem=rsem.at[source],
            device_id=peer_of(source, sect),
            device_id_type=pl.DeviceIdType.MESH,
        ).wait_recv()
        return carry

    lax.fori_loop(1, everyone, one, 0)


def wait_sent(send, recv, ssem, rsem, me, everyone, sect):
    def one(k, carry):
        message(send, recv, ssem, rsem, me, lax.rem(me + k, everyone), sect).wait_send()
        return carry

    lax.fori_loop(1, everyone, one, 0)


MIDDLE = 0.525
SCALE = 65536.0


def coded(values):
    return jnp.round((values - MIDDLE) * SCALE).astype(jnp.int32).astype(jnp.int16)


def decoded(values):
    return values.astype(jnp.int32).astype(jnp.float32) * (1.0 / SCALE) + MIDDLE


def spread_kernel(space, sect, d_ref, v_ref, x_ref, vo_ref, send, recv, vsend, vrecv, ssem, rsem, vssem, vrsem):
    planes, block, width = d_ref.shape
    everyone = space * sect
    mine, own = lax.axis_index("space"), lax.axis_index("sect")
    me = mine * sect + own
    barrier = greet(me, everyone, sect)
    columns = width // LANES

    def pack(c, carry):
        here = pl.ds(pl.multiple_of(c * LANES, LANES), LANES)
        for q in range(planes):
            left, right = swap_halves(d_ref[q, :ROWS, here], d_ref[q, ROWS:, here])
            send[2 * c, q] = coded(left)
            send[2 * c + 1, q] = coded(right)
        vsend[c, :planes, :] = v_ref[:, here]
        return carry

    lax.fori_loop(0, columns, pack, 0)
    pl.semaphore_wait(barrier, everyone - 1)

    def speeds(k, wait):
        other = lax.rem(mine + k, space)
        target = {"space": other, "sect": own}
        copy = pltpu.make_async_remote_copy(
            src_ref=vsend.at[(other * sect + own) // 2],
            dst_ref=vrecv.at[mine],
            send_sem=vssem.at[other],
            recv_sem=vrsem.at[mine],
            device_id=target,
            device_id_type=pl.DeviceIdType.MESH,
        )
        if wait:
            copy.wait_send()
            pltpu.make_async_remote_copy(
                src_ref=vsend.at[0],
                dst_ref=vrecv.at[other],
                send_sem=vssem.at[other],
                recv_sem=vrsem.at[other],
                device_id=target,
                device_id_type=pl.DeviceIdType.MESH,
            ).wait_recv()
        else:
            copy.start()

    for k in range(1, space):
        speeds(k, False)
    send_all(send, recv, ssem, rsem, me, everyone, sect)
    vrecv[mine] = vsend[me // 2]
    for k in range(1, space):
        speeds(k, True)
    even = lax.rem(own, 2) == 0
    for s in range(space // 2):
        a, b = vrecv[s], vrecv[s + space // 2]
        low, high = swap_halves(a, b)
        both = jnp.where(even, low, high)
        for q in range(planes):
            t = s * planes + q
            vo_ref[:, t * LANES : (t + 1) * LANES] = both[q : q + 1]
    wait_all(send, recv, ssem, rsem, me, everyone, sect)
    for s in range(space // 2):
        for z in range(sect):
            for q in range(planes):
                t = s * planes + q
                low, high = swap_halves(
                    decoded(recv[s * sect + z, q]),
                    decoded(recv[(s + space // 2) * sect + z, q]),
                )
                cols = slice(t * LANES, (t + 1) * LANES)
                x_ref[z * block : z * block + ROWS, cols] = low
                x_ref[z * block + ROWS : (z + 1) * block, cols] = high
    wait_sent(send, recv, ssem, rsem, me, everyone, sect)


def collect_kernel(space, sect, y_ref, o_ref, send, recv, ssem, rsem):
    planes, block, width = o_ref.shape
    everyone = space * sect
    me = lax.axis_index("space") * sect + lax.axis_index("sect")
    barrier = greet(me, everyone, sect)
    for s in range(space // 2):
        for z in range(sect):
            for q in range(planes):
                t = s * planes + q
                cols = slice(t * LANES, (t + 1) * LANES)
                low, high = swap_halves(
                    y_ref[z * block : z * block + ROWS, cols],
                    y_ref[z * block + ROWS : (z + 1) * block, cols],
                )
                send[s * sect + z, q] = low
                send[(s + space // 2) * sect + z, q] = high
    pl.semaphore_wait(barrier, everyone - 1)
    send_all(send, recv, ssem, rsem, me, everyone, sect)
    wait_all(send, recv, ssem, rsem, me, everyone, sect)

    def unpack(c, carry):
        here = pl.ds(pl.multiple_of(c * LANES, LANES), LANES)
        for q in range(planes):
            first, second = swap_halves(recv[2 * c, q], recv[2 * c + 1, q])
            o_ref[q, :ROWS, here] = first
            o_ref[q, ROWS:, here] = second
        return carry

    lax.fori_loop(0, width // LANES, unpack, 0)
    wait_sent(send, recv, ssem, rsem, me, everyone, sect)


def exchanged(density, velocity, kernel, split, target):
    planes, block, width = density.shape
    sections = kernel.shape[0]
    space, sect = lax.axis_size("space"), lax.axis_size("sect")
    everyone = space * sect
    cells = width // everyone * planes * space
    vmem = pl.BlockSpec(memory_space=pltpu.VMEM)
    packet = [pltpu.VMEM((everyone, planes, ROWS, LANES), kind) for kind in (jnp.int16, jnp.float32)]

    x, v = pl.pallas_call(
        lambda *refs: spread_kernel(space, sect, *refs),
        out_shape=(
            jax.ShapeDtypeStruct((sections, cells), jnp.float32),
            jax.ShapeDtypeStruct((1, cells), jnp.float32),
        ),
        in_specs=[vmem] * 2,
        out_specs=(vmem, vmem),
        scratch_shapes=[
            packet[0],
            packet[0],
            pltpu.VMEM((width // LANES, 8, LANES), jnp.float32),
            pltpu.VMEM((space, 8, LANES), jnp.float32),
            pltpu.SemaphoreType.DMA((everyone,)),
            pltpu.SemaphoreType.DMA((everyone,)),
            pltpu.SemaphoreType.DMA((space,)),
            pltpu.SemaphoreType.DMA((space,)),
        ],
        compiler_params=pltpu.CompilerParams(collective_id=0, has_side_effects=True),
        name="spread",
    )(density, velocity)
    y = compute(x, v, kernel, split, target, width // everyone)
    return pl.pallas_call(
        lambda *refs: collect_kernel(space, sect, *refs),
        out_shape=jax.ShapeDtypeStruct((planes, block, width), jnp.float32),
        in_specs=[vmem],
        out_specs=vmem,
        scratch_shapes=[
            packet[1],
            packet[1],
            pltpu.SemaphoreType.DMA((everyone,)),
            pltpu.SemaphoreType.DMA((everyone,)),
        ],
        compiler_params=pltpu.CompilerParams(collective_id=1, has_side_effects=True),
        name="collect",
    )(y)


def on_device(density, velocity, kernel, split, target):
    planes, block, width = density.shape
    sections = kernel.shape[0]
    space, sect = lax.axis_size("space"), lax.axis_size("sect")
    everyone = space * sect
    share = width // everyone
    groups = LANES // share
    tiles = planes * space // groups
    axes = ("space", "sect")
    if 2 * share == LANES and block == 2 * ROWS and space % 2 == 0 and sect % 2 == 0 and planes <= 8:
        return exchanged(density, velocity, kernel, split, target)

    sent = density.reshape(planes, block, everyone, share).transpose(2, 0, 1, 3)
    got = lax.all_to_all(sent, axes, 0, 0, tiled=True)
    got = got.reshape(space, sect, planes, block, share).transpose(1, 3, 0, 2, 4)
    got = got.reshape(sections, groups, tiles, share).transpose(0, 2, 1, 3)
    x = got.reshape(sections, tiles * LANES)

    vsent = velocity.reshape(planes, space, width // space).transpose(1, 0, 2)
    vgot = lax.all_to_all(vsent, "space", 0, 0, tiled=True).reshape(planes * space, width // space)
    v = lax.dynamic_slice_in_dim(vgot, lax.axis_index("sect") * share, share, 1)
    v = v.reshape(groups, tiles, share).transpose(1, 0, 2).reshape(1, tiles * LANES)

    y = compute(x, v, kernel, split, target, share)

    y = y.reshape(sections, tiles, groups, share).transpose(0, 2, 1, 3)
    y = y.reshape(sect, block, space, planes, share).transpose(2, 0, 3, 1, 4)
    y = y.reshape(everyone, planes, block, share)
    back = lax.all_to_all(y, axes, 0, 0, tiled=True)
    return back.transpose(1, 2, 0, 3).reshape(planes, block, width)


def solution(mesh):
    def run(*arrays):
        placed = (P("space", "sect", None), P("space", None), P(), P(), P())
        return jax.shard_map(
            on_device, mesh=mesh, in_specs=placed, out_specs=P("space", "sect", None), check_vma=False
        )(*arrays)

    def traced(*arrays):
        with jax.sharding.use_abstract_mesh(mesh.abstract_mesh):
            return run(*arrays)

    return traced
```

```python
import jax
import jax.numpy as jnp
from jax import lax
from jax.experimental import pallas as pl
from jax.experimental.pallas import tpu as pltpu
from jax.sharding import PartitionSpec as P

STEPS = 4
LANES = 128
ROWS = 16
DEEP = 256


def unit_list(sections):
    blocks = sections // ROWS
    units = [(0, i, None) for i in range(ROWS)]
    for b in range(1, blocks // 2):
        units += [(b, ROWS * b + r, ROWS * (blocks - b) + r) for r in range(ROWS)]
    half = blocks // 2
    units += [(half, ROWS * half + r, ROWS * half + ROWS // 2 + r) for r in range(ROWS // 2)]
    return units


def fold_tables(table, share, sections):
    blocks = sections // ROWS
    lane = lax.broadcasted_iota(jnp.int32, (ROWS, sections), 1)
    pieces = [table[:ROWS]]
    for b in range(1, blocks // 2):
        near = table[ROWS * b : ROWS * (b + 1)]
        far = table[ROWS * (blocks - b) : ROWS * (blocks - b + 1)]
        pieces.append(jnp.where(lane < ROWS * b, pltpu.roll(far, ROWS * b, 1), near))
    half = blocks // 2
    near = table[ROWS * half : ROWS * half + ROWS // 2]
    far = table[ROWS * half + ROWS // 2 : ROWS * (half + 1)]
    pieces.append(
        jnp.where(lane[: ROWS // 2] < ROWS * half, pltpu.roll(far, ROWS * half, 1), near)
    )
    return jnp.concatenate(pieces, axis=0)


def build_coefficients(kernel_ref, split_ref, target_ref, tt, bb, ww, coef):
    sections = kernel_ref.shape[0]
    beta = 0.5 * (kernel_ref[...] + kernel_ref[...].T)
    weight = 0.5 * (split_ref[...] + split_ref[...].T)
    row = lax.broadcasted_iota(jnp.int32, (sections, sections), 0)
    col = lax.broadcasted_iota(jnp.int32, (sections, sections), 1)
    share = jnp.where(col > row, 1.0, jnp.where(col == row, 0.5, 0.0)) * beta
    tt[...] = fold_tables(target_ref[...], None, sections)
    bb[...] = fold_tables(share, None, sections)
    ww[...] = fold_tables(weight, None, sections)
    ks = lax.broadcasted_iota(jnp.int32, (sections, sections), 0)

    def one(tile, carry):
        for part in range(DEEP // sections):
            unit = tile * (DEEP // sections) + part
            t = tt[pl.ds(unit, 1), :]
            b = bb[pl.ds(unit, 1), :]
            w = ww[pl.ds(unit, 1), :]
            low = b * w
            high = b * (1.0 - w)
            value = jnp.where(ks == t, low, jnp.where(ks == t + 1, high, 0.0))
            coef[tile, :, part * sections : (part + 1) * sections] = value.astype(jnp.bfloat16)
        return carry

    lax.fori_loop(0, coef.shape[0] - 1, one, 0)
    coef[coef.shape[0] - 1] = jnp.concatenate(
        [beta.astype(jnp.bfloat16), jnp.zeros((sections, sections), jnp.bfloat16)], axis=1
    )


def pair_tile(wide, low, tile, units, sections):
    blocks = []
    for part in range(DEEP // sections):
        b, near, far = units[tile * (DEEP // sections) + part]
        if far is not None:
            lead = jnp.broadcast_to(wide[far : far + 1, :], (ROWS, wide.shape[1])).astype(jnp.bfloat16)
            for start in range(sections - ROWS * b, sections, ROWS):
                blocks.append(lead * low[start : start + ROWS, :])
        lead = jnp.broadcast_to(wide[near : near + 1, :], (ROWS, wide.shape[1])).astype(jnp.bfloat16)
        for start in range(ROWS * b, sections, ROWS):
            blocks.append(lead * low[start : start + ROWS, :])
    return jnp.concatenate(blocks, axis=0)


def advance_all(state, speed, coef, tiles, shift):
    sections = state.shape[1]
    units = unit_list(sections)
    count = len(units) * sections // DEEP
    chunk = 2 * LANES if tiles % 2 == 0 else LANES
    engines = 2 if (tiles * LANES // chunk) % 2 == 0 else 1
    trips = tiles * LANES // (chunk * engines)

    def pads(slot):
        state[slot, :, :LANES] = pltpu.roll(
            state[slot, :, tiles * LANES : (tiles + 1) * LANES], shift % LANES, 1
        )
        state[slot, :, (tiles + 1) * LANES :] = pltpu.roll(
            state[slot, :, LANES : 2 * LANES], (LANES - shift) % LANES, 1
        )

    def finish(now, at, gain, rate):
        here = pl.ds(pl.multiple_of(at + LANES, LANES), chunk)
        before = pl.ds(pl.multiple_of(at, LANES), chunk)
        after = pl.ds(pl.multiple_of(at + 2 * LANES, LANES), chunk)
        s = state[now, :, here]
        v, u = speed[:, here], speed[:, before]
        flux = jnp.maximum(v, 0.0) * s + jnp.minimum(v, 0.0) * state[now, :, after]
        behind = jnp.maximum(u, 0.0) * state[now, :, before] + jnp.minimum(u, 0.0) * s
        state[1 - now, :, here] = s - (flux - behind) + (gain - s * rate)

    def step(index, carry):
        now = lax.rem(index, 2)
        pads(now)

        def trip(n, carry):
            def body():
                starts = [(n * engines + q) * chunk for q in range(engines)]
                wides, lows = [], []
                for q in range(engines):
                    here = pl.ds(pl.multiple_of(starts[q] + LANES, LANES), chunk)
                    wide = state.at[now, :, here]
                    wides.append(wide)
                    lows.append(wide[...].astype(jnp.bfloat16))
                for tile in range(count):
                    for q in range(engines):
                        rhs = pair_tile(wides[q], lows[q], tile, units, sections)
                        pltpu.matmul_push_rhs(rhs, staging_register=tile % 2, mxu_index=q)
                        pltpu.matmul_acc_lhs(accs[2 * q], coef[tile], load_staged_rhs=tile % 2)
                for q in range(engines):
                    rhs = jnp.concatenate([lows[q]] * (DEEP // sections), axis=0)
                    pltpu.matmul_push_rhs(rhs, staging_register=count % 2, mxu_index=q)
                    pltpu.matmul_acc_lhs(accs[2 * q + 1], coef[count], load_staged_rhs=count % 2)
                for q in range(engines):
                    gain = pltpu.matmul_pop(accs[2 * q])
                    rate = pltpu.matmul_pop(accs[2 * q + 1])
                    finish(now, starts[q], gain, rate)

            def body_dot():
                start = n * chunk
                here = pl.ds(pl.multiple_of(start + LANES, LANES), chunk)
                wide = state.at[now, :, here]
                low = wide[...].astype(jnp.bfloat16)
                gain = jnp.zeros((sections, chunk), jnp.float32)
                for tile in range(count):
                    rhs = pair_tile(wide, low, tile, units, sections)
                    gain += jnp.dot(coef[tile], rhs, preferred_element_type=jnp.float32)
                rate = jnp.dot(
                    coef[count][:, :sections], low, preferred_element_type=jnp.float32
                )
                finish(now, start, gain, rate)

            if chunk == DEEP:
                body()
            else:
                body_dot()
            return carry

        lax.fori_loop(0, trips, trip, 0)
        return carry

    def every(*found):
        accs.extend(found)
        for acc in found:
            pltpu.matmul_pop(acc)
        lax.fori_loop(0, STEPS, step, 0)

    accs = []
    if chunk == DEEP:
        pl.run_scoped(
            every,
            *[
                pltpu.ACC(q)((sections, DEEP), jnp.float32)
                for q in range(engines)
                for _ in range(2)
            ],
        )
    else:
        every()


def compute_kernel(shift, x_ref, v_ref, kernel_ref, split_ref, target_ref, o_ref, state, speed, tt, bb, ww, coef):
    tiles = x_ref.shape[1] // LANES
    build_coefficients(kernel_ref, split_ref, target_ref, tt, bb, ww, coef)
    width = tiles * LANES
    state[0, :, LANES : LANES + width] = x_ref[...]
    speed[:, LANES : LANES + width] = v_ref[...]
    speed[:, :LANES] = pltpu.roll(v_ref[:, width - LANES :], shift % LANES, 1)
    speed[:, LANES + width :] = pltpu.roll(v_ref[:, :LANES], (LANES - shift) % LANES, 1)
    advance_all(state, speed, coef, tiles, shift)
    o_ref[...] = state[STEPS % 2, :, LANES : LANES + width]


def compute(x, v, kernel, split, target, shift):
    sections, width = x.shape
    units = len(unit_list(sections))
    vmem = pl.BlockSpec(memory_space=pltpu.VMEM)

    def call(*refs):
        compute_kernel(shift, *refs)

    return pl.pallas_call(
        call,
        out_shape=jax.ShapeDtypeStruct((sections, width), jnp.float32),
        in_specs=[vmem] * 5,
        out_specs=vmem,
        scratch_shapes=[
            pltpu.VMEM((2, sections, width + 2 * LANES), jnp.float32),
            pltpu.VMEM((1, width + 2 * LANES), jnp.float32),
            pltpu.VMEM((units, sections), jnp.int32),
            pltpu.VMEM((units, sections), jnp.float32),
            pltpu.VMEM((units, sections), jnp.float32),
            pltpu.VMEM((units * sections // DEEP + 1, sections, DEEP), jnp.bfloat16),
        ],
        name="coagulate",
    )(x, v, kernel, split, target)


def swap_halves(first, second):
    half = LANES // 2
    left = lax.broadcasted_iota(jnp.int32, first.shape, 1) < half
    return (
        jnp.where(left, first, pltpu.roll(second, half, 1)),
        jnp.where(left, pltpu.roll(first, half, 1), second),
    )


def peer_of(index, sect):
    return {"space": index // sect, "sect": lax.rem(index, sect)}


def greet(me, everyone, sect):
    barrier = pltpu.get_barrier_semaphore()

    def one(k, carry):
        pl.semaphore_signal(
            barrier,
            inc=1,
            device_id=peer_of(lax.rem(me + k, everyone), sect),
            device_id_type=pl.DeviceIdType.MESH,
        )
        return carry

    lax.fori_loop(1, everyone, one, 0)
    return barrier


def message(send, recv, ssem, rsem, me, peer, sect):
    return pltpu.make_async_remote_copy(
        src_ref=send.at[peer],
        dst_ref=recv.at[me],
        send_sem=ssem.at[peer],
        recv_sem=rsem.at[me],
        device_id=peer_of(peer, sect),
        device_id_type=pl.DeviceIdType.MESH,
    )


def send_all(send, recv, ssem, rsem, me, everyone, sect):
    def one(k, carry):
        message(send, recv, ssem, rsem, me, lax.rem(me + k, everyone), sect).start()
        return carry

    lax.fori_loop(1, everyone, one, 0)
    recv[me] = send[me]


def wait_all(send, recv, ssem, rsem, me, everyone, sect):
    def one(k, carry):
        source = lax.rem(me + everyone - k, everyone)
        pltpu.make_async_remote_copy(
            src_ref=send.at[source],
            dst_ref=recv.at[source],
            send_sem=ssem.at[source],
            recv_sem=rsem.at[source],
            device_id=peer_of(source, sect),
            device_id_type=pl.DeviceIdType.MESH,
        ).wait_recv()
        return carry

    lax.fori_loop(1, everyone, one, 0)


def wait_sent(send, recv, ssem, rsem, me, everyone, sect):
    def one(k, carry):
        message(send, recv, ssem, rsem, me, lax.rem(me + k, everyone), sect).wait_send()
        return carry

    lax.fori_loop(1, everyone, one, 0)


MIDDLE = 0.525
SCALE = 65536.0


def coded(values):
    return jnp.round((values - MIDDLE) * SCALE).astype(jnp.int32).astype(jnp.int16)


def decoded(values):
    return values.astype(jnp.int32).astype(jnp.float32) * (1.0 / SCALE) + MIDDLE


FLOOR = 0.03
STEEP = 915.0 / 0.6931471805599453


def coded_result(values):
    code = jnp.log(1.0 + jnp.abs(values) * (1.0 / FLOOR)) * STEEP
    return jnp.round(jnp.where(values < 0.0, -code, code)).astype(jnp.int32).astype(jnp.int16)


def decoded_result(values):
    code = values.astype(jnp.int32).astype(jnp.float32)
    size = (jnp.exp(jnp.abs(code) * (1.0 / STEEP)) - 1.0) * FLOOR
    return jnp.where(code < 0.0, -size, size)


def fused_kernel(
    space, sect, shift,
    d_ref, v_ref, kernel_ref, split_ref, target_ref, back,
    state, speed, tt, bb, ww, coef, send, recv, vsend, vrecv, ssem, rsem, vssem, vrsem, ssem2, rsem2,
):
    planes, block, width = d_ref.shape
    everyone = space * sect
    mine, own = lax.axis_index("space"), lax.axis_index("sect")
    me = mine * sect + own
    barrier = greet(me, everyone, sect)
    columns = width // LANES

    def pack(c, carry):
        here = pl.ds(pl.multiple_of(c * LANES, LANES), LANES)
        for q in range(planes):
            left, right = swap_halves(d_ref[q, :ROWS, here], d_ref[q, ROWS:, here])
            send[2 * c, q] = coded(left)
            send[2 * c + 1, q] = coded(right)
        vsend[c, :planes, :] = v_ref[:, here]
        return carry

    lax.fori_loop(0, columns, pack, 0)
    pl.semaphore_wait(barrier, everyone - 1)

    def speeds(k, wait):
        other = lax.rem(mine + k, space)
        target = {"space": other, "sect": own}
        copy = pltpu.make_async_remote_copy(
            src_ref=vsend.at[(other * sect + own) // 2],
            dst_ref=vrecv.at[mine],
            send_sem=vssem.at[other],
            recv_sem=vrsem.at[mine],
            device_id=target,
            device_id_type=pl.DeviceIdType.MESH,
        )
        if wait:
            copy.wait_send()
            pltpu.make_async_remote_copy(
                src_ref=vsend.at[0],
                dst_ref=vrecv.at[other],
                send_sem=vssem.at[other],
                recv_sem=vrsem.at[other],
                device_id=target,
                device_id_type=pl.DeviceIdType.MESH,
            ).wait_recv()
        else:
            copy.start()

    send_all(send, recv, ssem, rsem, me, everyone, sect)
    for k in range(1, space):
        speeds(k, False)
    vrecv[mine] = vsend[me // 2]
    build_coefficients(kernel_ref, split_ref, target_ref, tt, bb, ww, coef)
    for k in range(1, space):
        speeds(k, True)
    even = lax.rem(own, 2) == 0
    for s in range(space // 2):
        low, high = swap_halves(vrecv[s], vrecv[s + space // 2])
        both = jnp.where(even, low, high)
        for q in range(planes):
            t = s * planes + q + 1
            speed[:, t * LANES : (t + 1) * LANES] = both[q : q + 1]
    tiles = planes * space // 2
    speed[:, :LANES] = pltpu.roll(speed[:, tiles * LANES : (tiles + 1) * LANES], shift, 1)
    speed[:, (tiles + 1) * LANES :] = pltpu.roll(speed[:, LANES : 2 * LANES], shift, 1)

    wait_all(send, recv, ssem, rsem, me, everyone, sect)
    for s in range(space // 2):
        for z in range(sect):
            for q in range(planes):
                t = s * planes + q + 1
                low, high = swap_halves(
                    decoded(recv[s * sect + z, q]),
                    decoded(recv[(s + space // 2) * sect + z, q]),
                )
                cols = slice(t * LANES, (t + 1) * LANES)
                state[0, z * block : z * block + ROWS, cols] = low
                state[0, z * block + ROWS : (z + 1) * block, cols] = high
    wait_sent(send, recv, ssem, rsem, me, everyone, sect)

    advance_all(state, speed, coef, tiles, shift)

    for s in range(space // 2):
        for z in range(sect):
            for q in range(planes):
                t = s * planes + q + 1
                cols = slice(t * LANES, (t + 1) * LANES)
                low, high = swap_halves(
                    state[STEPS % 2, z * block : z * block + ROWS, cols],
                    state[STEPS % 2, z * block + ROWS : (z + 1) * block, cols],
                )
                send[s * sect + z, q] = coded_result(low)
                send[(s + space // 2) * sect + z, q] = coded_result(high)
    send_all(send, back, ssem2, rsem2, me, everyone, sect)
    wait_all(send, back, ssem2, rsem2, me, everyone, sect)
    wait_sent(send, back, ssem2, rsem2, me, everyone, sect)


def unpack_kernel(got, o_ref):
    planes = o_ref.shape[0]
    for c in range(o_ref.shape[2] // LANES):
        here = slice(c * LANES, (c + 1) * LANES)
        for q in range(planes):
            first, second = swap_halves(decoded_result(got[2 * c, q]), decoded_result(got[2 * c + 1, q]))
            o_ref[q, :ROWS, here] = first
            o_ref[q, ROWS:, here] = second


def exchanged(density, velocity, kernel, split, target):
    planes, block, width = density.shape
    sections = kernel.shape[0]
    space, sect = lax.axis_size("space"), lax.axis_size("sect")
    everyone = space * sect
    share = width // everyone
    cells = share * planes * space
    units = len(unit_list(sections))
    vmem = pl.BlockSpec(memory_space=pltpu.VMEM)
    packet = (everyone, planes, ROWS, LANES)

    got = pl.pallas_call(
        lambda *refs: fused_kernel(space, sect, share, *refs),
        out_shape=jax.ShapeDtypeStruct(packet, jnp.int16),
        in_specs=[vmem] * 5,
        out_specs=vmem,
        scratch_shapes=[
            pltpu.VMEM((2, sections, cells + 2 * LANES), jnp.float32),
            pltpu.VMEM((1, cells + 2 * LANES), jnp.float32),
            pltpu.VMEM((units, sections), jnp.int32),
            pltpu.VMEM((units, sections), jnp.float32),
            pltpu.VMEM((units, sections), jnp.float32),
            pltpu.VMEM((units * sections // DEEP + 1, sections, DEEP), jnp.bfloat16),
            pltpu.VMEM(packet, jnp.int16),
            pltpu.VMEM(packet, jnp.int16),
            pltpu.VMEM((width // LANES, 8, LANES), jnp.float32),
            pltpu.VMEM((space, 8, LANES), jnp.float32),
            pltpu.SemaphoreType.DMA((everyone,)),
            pltpu.SemaphoreType.DMA((everyone,)),
            pltpu.SemaphoreType.DMA((space,)),
            pltpu.SemaphoreType.DMA((space,)),
            pltpu.SemaphoreType.DMA((everyone,)),
            pltpu.SemaphoreType.DMA((everyone,)),
        ],
        compiler_params=pltpu.CompilerParams(collective_id=0, has_side_effects=True),
        name="soot",
    )(density, velocity, kernel, split, target)
    half = width // 2
    return pl.pallas_call(
        unpack_kernel,
        grid=(2,),
        out_shape=jax.ShapeDtypeStruct((planes, block, width), jnp.float32),
        in_specs=[pl.BlockSpec((everyone // 2, planes, ROWS, LANES), lambda i: (i, 0, 0, 0))],
        out_specs=pl.BlockSpec((planes, block, half), lambda i: (0, 0, i)),
        name="unpack",
    )(got)


def on_device(density, velocity, kernel, split, target):
    planes, block, width = density.shape
    sections = kernel.shape[0]
    space, sect = lax.axis_size("space"), lax.axis_size("sect")
    everyone = space * sect
    share = width // everyone
    groups = LANES // share
    tiles = planes * space // groups
    axes = ("space", "sect")
    if 2 * share == LANES and block == 2 * ROWS and space % 2 == 0 and sect % 2 == 0 and planes <= 8:
        return exchanged(density, velocity, kernel, split, target)

    sent = density.reshape(planes, block, everyone, share).transpose(2, 0, 1, 3)
    got = lax.all_to_all(sent, axes, 0, 0, tiled=True)
    got = got.reshape(space, sect, planes, block, share).transpose(1, 3, 0, 2, 4)
    got = got.reshape(sections, groups, tiles, share).transpose(0, 2, 1, 3)
    x = got.reshape(sections, tiles * LANES)

    vsent = velocity.reshape(planes, space, width // space).transpose(1, 0, 2)
    vgot = lax.all_to_all(vsent, "space", 0, 0, tiled=True).reshape(planes * space, width // space)
    v = lax.dynamic_slice_in_dim(vgot, lax.axis_index("sect") * share, share, 1)
    v = v.reshape(groups, tiles, share).transpose(1, 0, 2).reshape(1, tiles * LANES)

    y = compute(x, v, kernel, split, target, share)

    y = y.reshape(sections, tiles, groups, share).transpose(0, 2, 1, 3)
    y = y.reshape(sect, block, space, planes, share).transpose(2, 0, 3, 1, 4)
    y = y.reshape(everyone, planes, block, share)
    back = lax.all_to_all(y, axes, 0, 0, tiled=True)
    return back.transpose(1, 2, 0, 3).reshape(planes, block, width)


def solution(mesh):
    def run(*arrays):
        placed = (P("space", "sect", None), P("space", None), P(), P(), P())
        return jax.shard_map(
            on_device, mesh=mesh, in_specs=placed, out_specs=P("space", "sect", None), check_vma=False
        )(*arrays)

    def traced(*arrays):
        with jax.sharding.use_abstract_mesh(mesh.abstract_mesh):
            return run(*arrays)

    return traced
```

```python
import jax
import jax.numpy as jnp
from jax import lax
from jax.experimental import pallas as pl
from jax.experimental.pallas import tpu as pltpu
from jax.sharding import PartitionSpec as P

STEPS = 4
LANES = 128
ROWS = 16
DEEP = 256


def unit_list(sections):
    blocks = sections // ROWS
    units = [(0, i, None) for i in range(ROWS)]
    for b in range(1, blocks // 2):
        units += [(b, ROWS * b + r, ROWS * (blocks - b) + r) for r in range(ROWS)]
    half = blocks // 2
    units += [(half, ROWS * half + r, ROWS * half + ROWS // 2 + r) for r in range(ROWS // 2)]
    return units


def fold_tables(table, share, sections):
    blocks = sections // ROWS
    lane = lax.broadcasted_iota(jnp.int32, (ROWS, sections), 1)
    pieces = [table[:ROWS]]
    for b in range(1, blocks // 2):
        near = table[ROWS * b : ROWS * (b + 1)]
        far = table[ROWS * (blocks - b) : ROWS * (blocks - b + 1)]
        pieces.append(jnp.where(lane < ROWS * b, pltpu.roll(far, ROWS * b, 1), near))
    half = blocks // 2
    near = table[ROWS * half : ROWS * half + ROWS // 2]
    far = table[ROWS * half + ROWS // 2 : ROWS * (half + 1)]
    pieces.append(
        jnp.where(lane[: ROWS // 2] < ROWS * half, pltpu.roll(far, ROWS * half, 1), near)
    )
    return jnp.concatenate(pieces, axis=0)


def build_coefficients(kernel_ref, split_ref, target_ref, tt, bb, ww, coef):
    sections = kernel_ref.shape[0]
    beta = 0.5 * (kernel_ref[...] + kernel_ref[...].T)
    weight = 0.5 * (split_ref[...] + split_ref[...].T)
    row = lax.broadcasted_iota(jnp.int32, (sections, sections), 0)
    col = lax.broadcasted_iota(jnp.int32, (sections, sections), 1)
    share = jnp.where(col > row, 1.0, jnp.where(col == row, 0.5, 0.0)) * beta
    tt[...] = fold_tables(target_ref[...], None, sections)
    bb[...] = fold_tables(share, None, sections)
    ww[...] = fold_tables(weight, None, sections)
    ks = lax.broadcasted_iota(jnp.int32, (sections, sections), 0)

    def one(tile, carry):
        for part in range(DEEP // sections):
            unit = tile * (DEEP // sections) + part
            t = tt[pl.ds(unit, 1), :]
            b = bb[pl.ds(unit, 1), :]
            w = ww[pl.ds(unit, 1), :]
            low = b * w
            high = b * (1.0 - w)
            value = jnp.where(ks == t, low, jnp.where(ks == t + 1, high, 0.0))
            coef[tile, :, part * sections : (part + 1) * sections] = value.astype(jnp.bfloat16)
        return carry

    lax.fori_loop(0, coef.shape[0] - 1, one, 0)
    coef[coef.shape[0] - 1] = jnp.concatenate(
        [beta.astype(jnp.bfloat16), jnp.zeros((sections, sections), jnp.bfloat16)], axis=1
    )


def pair_tile(wide, low, tile, units, sections):
    blocks = []
    for part in range(DEEP // sections):
        b, near, far = units[tile * (DEEP // sections) + part]
        if far is not None:
            lead = jnp.broadcast_to(wide[far : far + 1, :], (ROWS, wide.shape[1])).astype(jnp.bfloat16)
            for start in range(sections - ROWS * b, sections, ROWS):
                blocks.append(lead * low[start : start + ROWS, :])
        lead = jnp.broadcast_to(wide[near : near + 1, :], (ROWS, wide.shape[1])).astype(jnp.bfloat16)
        for start in range(ROWS * b, sections, ROWS):
            blocks.append(lead * low[start : start + ROWS, :])
    return jnp.concatenate(blocks, axis=0)


def advance_all(state, fresh, speed, coef, tiles, shift):
    sections = state.shape[0]
    units = unit_list(sections)
    count = len(units) * sections // DEEP
    chunk = 2 * LANES if tiles % 2 == 0 else LANES
    engines = 2 if (tiles * LANES // chunk) % 2 == 0 else 1
    trips = tiles * LANES // (chunk * engines)
    width = tiles * LANES

    def pads():
        state[:, :LANES] = pltpu.roll(state[:, width : width + LANES], shift % LANES, 1)
        state[:, width + LANES :] = pltpu.roll(state[:, LANES : 2 * LANES], (LANES - shift) % LANES, 1)

    def finish(at, gain, rate):
        here = slice(at + LANES, at + LANES + chunk)
        before = slice(at, at + chunk)
        after = slice(at + 2 * LANES, at + 2 * LANES + chunk)
        s = state[:, here]
        v, u = speed[:, here], speed[:, before]
        flux = jnp.maximum(v, 0.0) * s + jnp.minimum(v, 0.0) * state[:, after]
        behind = jnp.maximum(u, 0.0) * state[:, before] + jnp.minimum(u, 0.0) * s
        fresh[:, before] = s - (flux - behind) + (gain - s * rate)

    def trip(n):
        starts = [(n * engines + q) * chunk for q in range(engines)]
        wides = [state.at[:, at + LANES : at + LANES + chunk] for at in starts]
        lows = [wide[...].astype(jnp.bfloat16) for wide in wides]
        sums = accs[n % 2]
        for tile in range(count):
            for q in range(engines):
                rhs = pair_tile(wides[q], lows[q], tile, units, sections)
                pltpu.matmul_push_rhs(rhs, staging_register=tile % 2, mxu_index=q)
                pltpu.matmul_acc_lhs(sums[2 * q], coef[tile], load_staged_rhs=tile % 2)
        for q in range(engines):
            rhs = jnp.concatenate([lows[q]] * (DEEP // sections), axis=0)
            pltpu.matmul_push_rhs(rhs, staging_register=count % 2, mxu_index=q)
            pltpu.matmul_acc_lhs(sums[2 * q + 1], coef[count], load_staged_rhs=count % 2)
        for q in range(engines):
            finish(starts[q], pltpu.matmul_pop(sums[2 * q]), pltpu.matmul_pop(sums[2 * q + 1]))

    def trip_dot(n):
        start = n * chunk
        wide = state.at[:, start + LANES : start + LANES + chunk]
        low = wide[...].astype(jnp.bfloat16)
        gain = jnp.zeros((sections, chunk), jnp.float32)
        for tile in range(count):
            rhs = pair_tile(wide, low, tile, units, sections)
            gain += jnp.dot(coef[tile], rhs, preferred_element_type=jnp.float32)
        rate = jnp.dot(coef[count][:, :sections], low, preferred_element_type=jnp.float32)
        finish(start, gain, rate)

    def step(index, carry):
        pads()
        for n in range(trips):
            (trip if chunk == DEEP else trip_dot)(n)
        state[:, LANES : LANES + width] = fresh[...]
        return carry

    def every(*found):
        for acc in found:
            pltpu.matmul_pop(acc)
        accs.extend([found[: 2 * engines], found[2 * engines :]])
        lax.fori_loop(0, STEPS, step, 0)

    accs = []
    if chunk == DEEP:
        pl.run_scoped(
            every,
            *[
                pltpu.ACC(q)((sections, DEEP), jnp.float32)
                for _ in range(2)
                for q in range(engines)
                for _ in range(2)
            ],
        )
    else:
        every()


def compute_kernel(shift, x_ref, v_ref, kernel_ref, split_ref, target_ref, o_ref, state, fresh, speed, tt, bb, ww, coef):
    tiles = x_ref.shape[1] // LANES
    build_coefficients(kernel_ref, split_ref, target_ref, tt, bb, ww, coef)
    width = tiles * LANES
    state[:, LANES : LANES + width] = x_ref[...]
    speed[:, LANES : LANES + width] = v_ref[...]
    speed[:, :LANES] = pltpu.roll(v_ref[:, width - LANES :], shift % LANES, 1)
    speed[:, LANES + width :] = pltpu.roll(v_ref[:, :LANES], (LANES - shift) % LANES, 1)
    advance_all(state, fresh, speed, coef, tiles, shift)
    o_ref[...] = fresh[...]


def compute(x, v, kernel, split, target, shift):
    sections, width = x.shape
    units = len(unit_list(sections))
    vmem = pl.BlockSpec(memory_space=pltpu.VMEM)

    def call(*refs):
        compute_kernel(shift, *refs)

    return pl.pallas_call(
        call,
        out_shape=jax.ShapeDtypeStruct((sections, width), jnp.float32),
        in_specs=[vmem] * 5,
        out_specs=vmem,
        scratch_shapes=[
            pltpu.VMEM((sections, width + 2 * LANES), jnp.float32),
            pltpu.VMEM((sections, width), jnp.float32),
            pltpu.VMEM((1, width + 2 * LANES), jnp.float32),
            pltpu.VMEM((units, sections), jnp.int32),
            pltpu.VMEM((units, sections), jnp.float32),
            pltpu.VMEM((units, sections), jnp.float32),
            pltpu.VMEM((units * sections // DEEP + 1, sections, DEEP), jnp.bfloat16),
        ],
        name="coagulate",
    )(x, v, kernel, split, target)


def swap_halves(first, second):
    half = LANES // 2
    left = lax.broadcasted_iota(jnp.int32, first.shape, 1) < half
    return (
        jnp.where(left, first, pltpu.roll(second, half, 1)),
        jnp.where(left, pltpu.roll(first, half, 1), second),
    )


def peer_of(index, sect):
    return {"space": index // sect, "sect": lax.rem(index, sect)}


def greet(me, everyone, sect):
    barrier = pltpu.get_barrier_semaphore()

    def one(k, carry):
        pl.semaphore_signal(
            barrier,
            inc=1,
            device_id=peer_of(lax.rem(me + k, everyone), sect),
            device_id_type=pl.DeviceIdType.MESH,
        )
        return carry

    lax.fori_loop(1, everyone, one, 0)
    return barrier


def message(send, recv, ssem, rsem, me, peer, sect):
    return pltpu.make_async_remote_copy(
        src_ref=send.at[peer],
        dst_ref=recv.at[me],
        send_sem=ssem.at[peer],
        recv_sem=rsem.at[me],
        device_id=peer_of(peer, sect),
        device_id_type=pl.DeviceIdType.MESH,
    )


def send_all(send, recv, ssem, rsem, me, everyone, sect):
    def one(k, carry):
        message(send, recv, ssem, rsem, me, lax.rem(me + k, everyone), sect).start()
        return carry

    lax.fori_loop(1, everyone, one, 0)
    recv[me] = send[me]


def wait_all(send, recv, ssem, rsem, me, everyone, sect):
    def one(k, carry):
        source = lax.rem(me + everyone - k, everyone)
        pltpu.make_async_remote_copy(
            src_ref=send.at[source],
            dst_ref=recv.at[source],
            send_sem=ssem.at[source],
            recv_sem=rsem.at[source],
            device_id=peer_of(source, sect),
            device_id_type=pl.DeviceIdType.MESH,
        ).wait_recv()
        return carry

    lax.fori_loop(1, everyone, one, 0)


def wait_sent(send, recv, ssem, rsem, me, everyone, sect):
    def one(k, carry):
        message(send, recv, ssem, rsem, me, lax.rem(me + k, everyone), sect).wait_send()
        return carry

    lax.fori_loop(1, everyone, one, 0)


MIDDLE = 0.525
SCALE = 65536.0


def coded(values):
    return jnp.round((values - MIDDLE) * SCALE).astype(jnp.int32).astype(jnp.int16)


def decoded(values):
    return values.astype(jnp.int32).astype(jnp.float32) * (1.0 / SCALE) + MIDDLE


FLOOR = 0.03
STEEP = 915.0 / 0.6931471805599453


def coded_result(values):
    code = jnp.log(1.0 + jnp.abs(values) * (1.0 / FLOOR)) * STEEP
    return jnp.round(jnp.where(values < 0.0, -code, code)).astype(jnp.int32).astype(jnp.int16)


def decoded_result(values):
    code = values.astype(jnp.int32).astype(jnp.float32)
    size = (jnp.exp(jnp.abs(code) * (1.0 / STEEP)) - 1.0) * FLOOR
    return jnp.where(code < 0.0, -size, size)


def fused_kernel(
    space, sect, shift,
    d_ref, v_ref, kernel_ref, split_ref, target_ref, back,
    state, fresh, speed, tt, bb, ww, coef, send, recv, vsend, vrecv, ssem, rsem, vssem, vrsem, ssem2, rsem2,
):
    planes, block, width = d_ref.shape
    everyone = space * sect
    mine, own = lax.axis_index("space"), lax.axis_index("sect")
    me = mine * sect + own
    barrier = greet(me, everyone, sect)
    columns = width // LANES

    def pack(c, carry):
        here = pl.ds(pl.multiple_of(c * LANES, LANES), LANES)
        for q in range(planes):
            left, right = swap_halves(d_ref[q, :ROWS, here], d_ref[q, ROWS:, here])
            send[2 * c, q] = coded(left)
            send[2 * c + 1, q] = coded(right)
        vsend[c, :planes, :] = v_ref[:, here]
        return carry

    lax.fori_loop(0, columns, pack, 0)
    pl.semaphore_wait(barrier, everyone - 1)

    def speeds(k, wait):
        other = lax.rem(mine + k, space)
        target = {"space": other, "sect": own}
        copy = pltpu.make_async_remote_copy(
            src_ref=vsend.at[(other * sect + own) // 2],
            dst_ref=vrecv.at[mine],
            send_sem=vssem.at[other],
            recv_sem=vrsem.at[mine],
            device_id=target,
            device_id_type=pl.DeviceIdType.MESH,
        )
        if wait:
            copy.wait_send()
            pltpu.make_async_remote_copy(
                src_ref=vsend.at[0],
                dst_ref=vrecv.at[other],
                send_sem=vssem.at[other],
                recv_sem=vrsem.at[other],
                device_id=target,
                device_id_type=pl.DeviceIdType.MESH,
            ).wait_recv()
        else:
            copy.start()

    send_all(send, recv, ssem, rsem, me, everyone, sect)
    for k in range(1, space):
        speeds(k, False)
    vrecv[mine] = vsend[me // 2]
    build_coefficients(kernel_ref, split_ref, target_ref, tt, bb, ww, coef)
    for k in range(1, space):
        speeds(k, True)
    even = lax.rem(own, 2) == 0
    for s in range(space // 2):
        low, high = swap_halves(vrecv[s], vrecv[s + space // 2])
        both = jnp.where(even, low, high)
        for q in range(planes):
            t = s * planes + q + 1
            speed[:, t * LANES : (t + 1) * LANES] = both[q : q + 1]
    tiles = planes * space // 2
    speed[:, :LANES] = pltpu.roll(speed[:, tiles * LANES : (tiles + 1) * LANES], shift, 1)
    speed[:, (tiles + 1) * LANES :] = pltpu.roll(speed[:, LANES : 2 * LANES], shift, 1)

    wait_all(send, recv, ssem, rsem, me, everyone, sect)
    for s in range(space // 2):
        for z in range(sect):
            for q in range(planes):
                t = s * planes + q + 1
                low, high = swap_halves(
                    decoded(recv[s * sect + z, q]),
                    decoded(recv[(s + space // 2) * sect + z, q]),
                )
                cols = slice(t * LANES, (t + 1) * LANES)
                state[z * block : z * block + ROWS, cols] = low
                state[z * block + ROWS : (z + 1) * block, cols] = high
    wait_sent(send, recv, ssem, rsem, me, everyone, sect)

    advance_all(state, fresh, speed, coef, tiles, shift)

    for s in range(space // 2):
        for z in range(sect):
            for q in range(planes):
                t = s * planes + q + 1
                cols = slice(t * LANES, (t + 1) * LANES)
                low, high = swap_halves(
                    state[z * block : z * block + ROWS, cols],
                    state[z * block + ROWS : (z + 1) * block, cols],
                )
                send[s * sect + z, q] = coded_result(low)
                send[(s + space // 2) * sect + z, q] = coded_result(high)
    send_all(send, back, ssem2, rsem2, me, everyone, sect)
    wait_all(send, back, ssem2, rsem2, me, everyone, sect)
    wait_sent(send, back, ssem2, rsem2, me, everyone, sect)


def unpack_kernel(got, o_ref):
    planes = o_ref.shape[0]
    for c in range(o_ref.shape[2] // LANES):
        here = slice(c * LANES, (c + 1) * LANES)
        for q in range(planes):
            first, second = swap_halves(decoded_result(got[2 * c, q]), decoded_result(got[2 * c + 1, q]))
            o_ref[q, :ROWS, here] = first
            o_ref[q, ROWS:, here] = second


def exchanged(density, velocity, kernel, split, target):
    planes, block, width = density.shape
    sections = kernel.shape[0]
    space, sect = lax.axis_size("space"), lax.axis_size("sect")
    everyone = space * sect
    share = width // everyone
    cells = share * planes * space
    units = len(unit_list(sections))
    vmem = pl.BlockSpec(memory_space=pltpu.VMEM)
    packet = (everyone, planes, ROWS, LANES)

    got = pl.pallas_call(
        lambda *refs: fused_kernel(space, sect, share, *refs),
        out_shape=jax.ShapeDtypeStruct(packet, jnp.int16),
        in_specs=[vmem] * 5,
        out_specs=vmem,
        scratch_shapes=[
            pltpu.VMEM((sections, cells + 2 * LANES), jnp.float32),
            pltpu.VMEM((sections, cells), jnp.float32),
            pltpu.VMEM((1, cells + 2 * LANES), jnp.float32),
            pltpu.VMEM((units, sections), jnp.int32),
            pltpu.VMEM((units, sections), jnp.float32),
            pltpu.VMEM((units, sections), jnp.float32),
            pltpu.VMEM((units * sections // DEEP + 1, sections, DEEP), jnp.bfloat16),
            pltpu.VMEM(packet, jnp.int16),
            pltpu.VMEM(packet, jnp.int16),
            pltpu.VMEM((width // LANES, 8, LANES), jnp.float32),
            pltpu.VMEM((space, 8, LANES), jnp.float32),
            pltpu.SemaphoreType.DMA((everyone,)),
            pltpu.SemaphoreType.DMA((everyone,)),
            pltpu.SemaphoreType.DMA((space,)),
            pltpu.SemaphoreType.DMA((space,)),
            pltpu.SemaphoreType.DMA((everyone,)),
            pltpu.SemaphoreType.DMA((everyone,)),
        ],
        compiler_params=pltpu.CompilerParams(collective_id=0, has_side_effects=True),
        name="soot",
    )(density, velocity, kernel, split, target)
    half = width // 2
    return pl.pallas_call(
        unpack_kernel,
        grid=(2,),
        out_shape=jax.ShapeDtypeStruct((planes, block, width), jnp.float32),
        in_specs=[pl.BlockSpec((everyone // 2, planes, ROWS, LANES), lambda i: (i, 0, 0, 0))],
        out_specs=pl.BlockSpec((planes, block, half), lambda i: (0, 0, i)),
        name="unpack",
    )(got)


def on_device(density, velocity, kernel, split, target):
    planes, block, width = density.shape
    sections = kernel.shape[0]
    space, sect = lax.axis_size("space"), lax.axis_size("sect")
    everyone = space * sect
    share = width // everyone
    groups = LANES // share
    tiles = planes * space // groups
    axes = ("space", "sect")
    if 2 * share == LANES and block == 2 * ROWS and space % 2 == 0 and sect % 2 == 0 and planes <= 8:
        return exchanged(density, velocity, kernel, split, target)

    sent = density.reshape(planes, block, everyone, share).transpose(2, 0, 1, 3)
    got = lax.all_to_all(sent, axes, 0, 0, tiled=True)
    got = got.reshape(space, sect, planes, block, share).transpose(1, 3, 0, 2, 4)
    got = got.reshape(sections, groups, tiles, share).transpose(0, 2, 1, 3)
    x = got.reshape(sections, tiles * LANES)

    vsent = velocity.reshape(planes, space, width // space).transpose(1, 0, 2)
    vgot = lax.all_to_all(vsent, "space", 0, 0, tiled=True).reshape(planes * space, width // space)
    v = lax.dynamic_slice_in_dim(vgot, lax.axis_index("sect") * share, share, 1)
    v = v.reshape(groups, tiles, share).transpose(1, 0, 2).reshape(1, tiles * LANES)

    y = compute(x, v, kernel, split, target, share)

    y = y.reshape(sections, tiles, groups, share).transpose(0, 2, 1, 3)
    y = y.reshape(sect, block, space, planes, share).transpose(2, 0, 3, 1, 4)
    y = y.reshape(everyone, planes, block, share)
    back = lax.all_to_all(y, axes, 0, 0, tiled=True)
    return back.transpose(1, 2, 0, 3).reshape(planes, block, width)


def solution(mesh):
    def run(*arrays):
        placed = (P("space", "sect", None), P("space", None), P(), P(), P())
        return jax.shard_map(
            on_device, mesh=mesh, in_specs=placed, out_specs=P("space", "sect", None), check_vma=False
        )(*arrays)

    def traced(*arrays):
        with jax.sharding.use_abstract_mesh(mesh.abstract_mesh):
            return run(*arrays)

    return traced
```

```python
import jax
import jax.numpy as jnp
from jax import lax
from jax.experimental import pallas as pl
from jax.experimental.pallas import tpu as pltpu
from jax.sharding import PartitionSpec as P

STEPS = 4
LANES = 128
ROWS = 16
DEEP = 256


def unit_list(sections):
    blocks = sections // ROWS
    units = [(0, i, None) for i in range(ROWS)]
    for b in range(1, blocks // 2):
        units += [(b, ROWS * b + r, ROWS * (blocks - b) + r) for r in range(ROWS)]
    half = blocks // 2
    units += [(half, ROWS * half + r, ROWS * half + ROWS // 2 + r) for r in range(ROWS // 2)]
    return units


def fold_tables(table, share, sections):
    blocks = sections // ROWS
    lane = lax.broadcasted_iota(jnp.int32, (ROWS, sections), 1)
    pieces = [table[:ROWS]]
    for b in range(1, blocks // 2):
        near = table[ROWS * b : ROWS * (b + 1)]
        far = table[ROWS * (blocks - b) : ROWS * (blocks - b + 1)]
        pieces.append(jnp.where(lane < ROWS * b, pltpu.roll(far, ROWS * b, 1), near))
    half = blocks // 2
    near = table[ROWS * half : ROWS * half + ROWS // 2]
    far = table[ROWS * half + ROWS // 2 : ROWS * (half + 1)]
    pieces.append(
        jnp.where(lane[: ROWS // 2] < ROWS * half, pltpu.roll(far, ROWS * half, 1), near)
    )
    return jnp.concatenate(pieces, axis=0)


def build_coefficients(kernel_ref, split_ref, target_ref, tt, bb, ww, coef):
    sections = kernel_ref.shape[0]
    beta = 0.5 * (kernel_ref[...] + kernel_ref[...].T)
    weight = 0.5 * (split_ref[...] + split_ref[...].T)
    row = lax.broadcasted_iota(jnp.int32, (sections, sections), 0)
    col = lax.broadcasted_iota(jnp.int32, (sections, sections), 1)
    share = jnp.where(col > row, 1.0, jnp.where(col == row, 0.5, 0.0)) * beta
    tt[...] = fold_tables(target_ref[...], None, sections)
    bb[...] = fold_tables(share, None, sections)
    ww[...] = fold_tables(weight, None, sections)
    ks = lax.broadcasted_iota(jnp.int32, (sections, sections), 0)

    def one(tile, carry):
        for part in range(DEEP // sections):
            unit = tile * (DEEP // sections) + part
            t = tt[pl.ds(unit, 1), :]
            b = bb[pl.ds(unit, 1), :]
            w = ww[pl.ds(unit, 1), :]
            low = b * w
            high = b * (1.0 - w)
            value = jnp.where(ks == t, low, jnp.where(ks == t + 1, high, 0.0))
            coef[tile, :, part * sections : (part + 1) * sections] = value.astype(jnp.bfloat16)
        return carry

    lax.fori_loop(0, coef.shape[0] - 1, one, 0)
    coef[coef.shape[0] - 1] = jnp.concatenate(
        [beta.astype(jnp.bfloat16), jnp.zeros((sections, sections), jnp.bfloat16)], axis=1
    )


def pair_tile(wide, low, tile, units, sections):
    blocks = []
    for part in range(DEEP // sections):
        b, near, far = units[tile * (DEEP // sections) + part]
        if far is not None:
            lead = jnp.broadcast_to(wide[far : far + 1, :], (ROWS, wide.shape[1])).astype(jnp.bfloat16)
            for start in range(sections - ROWS * b, sections, ROWS):
                blocks.append(lead * low[start : start + ROWS, :])
        lead = jnp.broadcast_to(wide[near : near + 1, :], (ROWS, wide.shape[1])).astype(jnp.bfloat16)
        for start in range(ROWS * b, sections, ROWS):
            blocks.append(lead * low[start : start + ROWS, :])
    return jnp.concatenate(blocks, axis=0)


def advance_all(state, fresh, speed, coef, tiles, shift, emit=None):
    sections = state.shape[0]
    units = unit_list(sections)
    count = len(units) * sections // DEEP
    chunk = 2 * LANES if tiles % 2 == 0 else LANES
    engines = 2 if (tiles * LANES // chunk) % 2 == 0 else 1
    trips = tiles * LANES // (chunk * engines)
    width = tiles * LANES

    def pads():
        state[:, :LANES] = pltpu.roll(state[:, width : width + LANES], shift % LANES, 1)
        state[:, width + LANES :] = pltpu.roll(state[:, LANES : 2 * LANES], (LANES - shift) % LANES, 1)

    def finish(at, gain, rate):
        here = slice(at + LANES, at + LANES + chunk)
        before = slice(at, at + chunk)
        after = slice(at + 2 * LANES, at + 2 * LANES + chunk)
        s = state[:, here]
        v, u = speed[:, here], speed[:, before]
        flux = jnp.maximum(v, 0.0) * s + jnp.minimum(v, 0.0) * state[:, after]
        behind = jnp.maximum(u, 0.0) * state[:, before] + jnp.minimum(u, 0.0) * s
        fresh[:, before] = s - (flux - behind) + (gain - s * rate)

    def trip(n):
        starts = [(n * engines + q) * chunk for q in range(engines)]
        wides = [state.at[:, at + LANES : at + LANES + chunk] for at in starts]
        lows = [wide[...].astype(jnp.bfloat16) for wide in wides]
        sums = accs[n % 2]
        for tile in range(count):
            for q in range(engines):
                rhs = pair_tile(wides[q], lows[q], tile, units, sections)
                pltpu.matmul_push_rhs(rhs, staging_register=tile % 2, mxu_index=q)
                pltpu.matmul_acc_lhs(sums[2 * q], coef[tile], load_staged_rhs=tile % 2)
        for q in range(engines):
            rhs = jnp.concatenate([lows[q]] * (DEEP // sections), axis=0)
            pltpu.matmul_push_rhs(rhs, staging_register=count % 2, mxu_index=q)
            pltpu.matmul_acc_lhs(sums[2 * q + 1], coef[count], load_staged_rhs=count % 2)
        for q in range(engines):
            finish(starts[q], pltpu.matmul_pop(sums[2 * q]), pltpu.matmul_pop(sums[2 * q + 1]))

    def trip_dot(n):
        start = n * chunk
        wide = state.at[:, start + LANES : start + LANES + chunk]
        low = wide[...].astype(jnp.bfloat16)
        gain = jnp.zeros((sections, chunk), jnp.float32)
        for tile in range(count):
            rhs = pair_tile(wide, low, tile, units, sections)
            gain += jnp.dot(coef[tile], rhs, preferred_element_type=jnp.float32)
        rate = jnp.dot(coef[count][:, :sections], low, preferred_element_type=jnp.float32)
        finish(start, gain, rate)

    def step(index, carry):
        pads()
        for n in range(trips):
            (trip if chunk == DEEP else trip_dot)(n)
        state[:, LANES : LANES + width] = fresh[...]
        return carry

    def every(*found):
        for acc in found:
            pltpu.matmul_pop(acc)
        accs.extend([found[: 2 * engines], found[2 * engines :]])
        lax.fori_loop(0, STEPS - 1, step, 0)
        pads()
        done = 0
        for n in range(trips):
            (trip if chunk == DEEP else trip_dot)(n)
            if emit is not None:
                done = emit(done, (n + 1) * engines * chunk // LANES)

    accs = []
    if chunk == DEEP:
        pl.run_scoped(
            every,
            *[
                pltpu.ACC(q)((sections, DEEP), jnp.float32)
                for _ in range(2)
                for q in range(engines)
                for _ in range(2)
            ],
        )
    else:
        every()


def compute_kernel(shift, x_ref, v_ref, kernel_ref, split_ref, target_ref, o_ref, state, fresh, speed, tt, bb, ww, coef):
    tiles = x_ref.shape[1] // LANES
    build_coefficients(kernel_ref, split_ref, target_ref, tt, bb, ww, coef)
    width = tiles * LANES
    state[:, LANES : LANES + width] = x_ref[...]
    speed[:, LANES : LANES + width] = v_ref[...]
    speed[:, :LANES] = pltpu.roll(v_ref[:, width - LANES :], shift % LANES, 1)
    speed[:, LANES + width :] = pltpu.roll(v_ref[:, :LANES], (LANES - shift) % LANES, 1)
    advance_all(state, fresh, speed, coef, tiles, shift)
    o_ref[...] = fresh[...]


def compute(x, v, kernel, split, target, shift):
    sections, width = x.shape
    units = len(unit_list(sections))
    vmem = pl.BlockSpec(memory_space=pltpu.VMEM)

    def call(*refs):
        compute_kernel(shift, *refs)

    return pl.pallas_call(
        call,
        out_shape=jax.ShapeDtypeStruct((sections, width), jnp.float32),
        in_specs=[vmem] * 5,
        out_specs=vmem,
        scratch_shapes=[
            pltpu.VMEM((sections, width + 2 * LANES), jnp.float32),
            pltpu.VMEM((sections, width), jnp.float32),
            pltpu.VMEM((1, width + 2 * LANES), jnp.float32),
            pltpu.VMEM((units, sections), jnp.int32),
            pltpu.VMEM((units, sections), jnp.float32),
            pltpu.VMEM((units, sections), jnp.float32),
            pltpu.VMEM((units * sections // DEEP + 1, sections, DEEP), jnp.bfloat16),
        ],
        name="coagulate",
    )(x, v, kernel, split, target)


def swap_halves(first, second):
    half = LANES // 2
    left = lax.broadcasted_iota(jnp.int32, first.shape, 1) < half
    return (
        jnp.where(left, first, pltpu.roll(second, half, 1)),
        jnp.where(left, pltpu.roll(first, half, 1), second),
    )


def peer_of(index, sect):
    return {"space": index // sect, "sect": lax.rem(index, sect)}


def greet(me, everyone, sect):
    barrier = pltpu.get_barrier_semaphore()

    def one(k, carry):
        pl.semaphore_signal(
            barrier,
            inc=1,
            device_id=peer_of(lax.rem(me + k, everyone), sect),
            device_id_type=pl.DeviceIdType.MESH,
        )
        return carry

    lax.fori_loop(1, everyone, one, 0)
    return barrier


def message(send, recv, ssem, rsem, me, peer, sect):
    return pltpu.make_async_remote_copy(
        src_ref=send.at[peer],
        dst_ref=recv.at[me],
        send_sem=ssem.at[peer],
        recv_sem=rsem.at[me],
        device_id=peer_of(peer, sect),
        device_id_type=pl.DeviceIdType.MESH,
    )


def send_all(send, recv, ssem, rsem, me, everyone, sect):
    def one(k, carry):
        message(send, recv, ssem, rsem, me, lax.rem(me + k, everyone), sect).start()
        return carry

    lax.fori_loop(1, everyone, one, 0)
    recv[me] = send[me]


def wait_all(send, recv, ssem, rsem, me, everyone, sect):
    def one(k, carry):
        source = lax.rem(me + everyone - k, everyone)
        pltpu.make_async_remote_copy(
            src_ref=send.at[source],
            dst_ref=recv.at[source],
            send_sem=ssem.at[source],
            recv_sem=rsem.at[source],
            device_id=peer_of(source, sect),
            device_id_type=pl.DeviceIdType.MESH,
        ).wait_recv()
        return carry

    lax.fori_loop(1, everyone, one, 0)


def wait_sent(send, recv, ssem, rsem, me, everyone, sect):
    def one(k, carry):
        message(send, recv, ssem, rsem, me, lax.rem(me + k, everyone), sect).wait_send()
        return carry

    lax.fori_loop(1, everyone, one, 0)


MIDDLE = 0.525
SCALE = 65536.0


def coded(values):
    return jnp.round((values - MIDDLE) * SCALE).astype(jnp.int32).astype(jnp.int16)


def decoded(values):
    return values.astype(jnp.int32).astype(jnp.float32) * (1.0 / SCALE) + MIDDLE


FLOOR = 0.03
STEEP = 915.0 / 0.6931471805599453


def coded_result(values):
    code = jnp.log(1.0 + jnp.abs(values) * (1.0 / FLOOR)) * STEEP
    return jnp.round(jnp.where(values < 0.0, -code, code)).astype(jnp.int32).astype(jnp.int16)


def decoded_result(values):
    code = values.astype(jnp.int32).astype(jnp.float32)
    size = (jnp.exp(jnp.abs(code) * (1.0 / STEEP)) - 1.0) * FLOOR
    return jnp.where(code < 0.0, -size, size)


def fused_kernel(
    space, sect, shift,
    d_ref, v_ref, kernel_ref, split_ref, target_ref, back,
    state, fresh, speed, tt, bb, ww, coef, send, recv, vsend, vrecv, ssem, rsem, vssem, vrsem, ssem2, rsem2,
):
    planes, block, width = d_ref.shape
    everyone = space * sect
    mine, own = lax.axis_index("space"), lax.axis_index("sect")
    me = mine * sect + own
    barrier = greet(me, everyone, sect)
    columns = width // LANES

    def pack(c, carry):
        here = pl.ds(pl.multiple_of(c * LANES, LANES), LANES)
        for q in range(planes):
            left, right = swap_halves(d_ref[q, :ROWS, here], d_ref[q, ROWS:, here])
            send[2 * c, q] = coded(left)
            send[2 * c + 1, q] = coded(right)
        vsend[c, :planes, :] = v_ref[:, here]
        return carry

    lax.fori_loop(0, columns, pack, 0)
    pl.semaphore_wait(barrier, everyone - 1)

    def speeds(k, wait):
        other = lax.rem(mine + k, space)
        target = {"space": other, "sect": own}
        copy = pltpu.make_async_remote_copy(
            src_ref=vsend.at[(other * sect + own) // 2],
            dst_ref=vrecv.at[mine],
            send_sem=vssem.at[other],
            recv_sem=vrsem.at[mine],
            device_id=target,
            device_id_type=pl.DeviceIdType.MESH,
        )
        if wait:
            copy.wait_send()
            pltpu.make_async_remote_copy(
                src_ref=vsend.at[0],
                dst_ref=vrecv.at[other],
                send_sem=vssem.at[other],
                recv_sem=vrsem.at[other],
                device_id=target,
                device_id_type=pl.DeviceIdType.MESH,
            ).wait_recv()
        else:
            copy.start()

    send_all(send, recv, ssem, rsem, me, everyone, sect)
    for k in range(1, space):
        speeds(k, False)
    vrecv[mine] = vsend[me // 2]
    build_coefficients(kernel_ref, split_ref, target_ref, tt, bb, ww, coef)
    for k in range(1, space):
        speeds(k, True)
    even = lax.rem(own, 2) == 0
    for s in range(space // 2):
        low, high = swap_halves(vrecv[s], vrecv[s + space // 2])
        both = jnp.where(even, low, high)
        for q in range(planes):
            t = s * planes + q + 1
            speed[:, t * LANES : (t + 1) * LANES] = both[q : q + 1]
    tiles = planes * space // 2
    speed[:, :LANES] = pltpu.roll(speed[:, tiles * LANES : (tiles + 1) * LANES], shift, 1)
    speed[:, (tiles + 1) * LANES :] = pltpu.roll(speed[:, LANES : 2 * LANES], shift, 1)

    wait_all(send, recv, ssem, rsem, me, everyone, sect)
    for s in range(space // 2):
        for z in range(sect):
            for q in range(planes):
                t = s * planes + q + 1
                low, high = swap_halves(
                    decoded(recv[s * sect + z, q]),
                    decoded(recv[(s + space // 2) * sect + z, q]),
                )
                cols = slice(t * LANES, (t + 1) * LANES)
                state[z * block : z * block + ROWS, cols] = low
                state[z * block + ROWS : (z + 1) * block, cols] = high
    wait_sent(send, recv, ssem, rsem, me, everyone, sect)

    def emit(done, ready):
        last = ready // planes
        for s in range(done, last):
            for z in range(sect):
                for q in range(planes):
                    t = s * planes + q
                    cols = slice(t * LANES, (t + 1) * LANES)
                    low, high = swap_halves(
                        fresh[z * block : z * block + ROWS, cols],
                        fresh[z * block + ROWS : (z + 1) * block, cols],
                    )
                    send[s * sect + z, q] = coded_result(low)
                    send[(s + space // 2) * sect + z, q] = coded_result(high)

        def one(k, carry):
            for first in (0, space // 2 * sect):
                peer = first + k

                @pl.when(peer != me)
                def _():
                    message(send, back, ssem2, rsem2, me, peer, sect).start()

            return carry

        lax.fori_loop(done * sect, last * sect, one, 0)
        return last

    advance_all(state, fresh, speed, coef, tiles, shift, emit)
    back[me] = send[me]
    wait_all(send, back, ssem2, rsem2, me, everyone, sect)
    wait_sent(send, back, ssem2, rsem2, me, everyone, sect)


def unpack_kernel(got, o_ref):
    planes = o_ref.shape[0]
    for c in range(o_ref.shape[2] // LANES):
        here = slice(c * LANES, (c + 1) * LANES)
        for q in range(planes):
            first, second = swap_halves(decoded_result(got[2 * c, q]), decoded_result(got[2 * c + 1, q]))
            o_ref[q, :ROWS, here] = first
            o_ref[q, ROWS:, here] = second


def exchanged(density, velocity, kernel, split, target):
    planes, block, width = density.shape
    sections = kernel.shape[0]
    space, sect = lax.axis_size("space"), lax.axis_size("sect")
    everyone = space * sect
    share = width // everyone
    cells = share * planes * space
    units = len(unit_list(sections))
    vmem = pl.BlockSpec(memory_space=pltpu.VMEM)
    packet = (everyone, planes, ROWS, LANES)

    got = pl.pallas_call(
        lambda *refs: fused_kernel(space, sect, share, *refs),
        out_shape=jax.ShapeDtypeStruct(packet, jnp.int16),
        in_specs=[vmem] * 5,
        out_specs=vmem,
        scratch_shapes=[
            pltpu.VMEM((sections, cells + 2 * LANES), jnp.float32),
            pltpu.VMEM((sections, cells), jnp.float32),
            pltpu.VMEM((1, cells + 2 * LANES), jnp.float32),
            pltpu.VMEM((units, sections), jnp.int32),
            pltpu.VMEM((units, sections), jnp.float32),
            pltpu.VMEM((units, sections), jnp.float32),
            pltpu.VMEM((units * sections // DEEP + 1, sections, DEEP), jnp.bfloat16),
            pltpu.VMEM(packet, jnp.int16),
            pltpu.VMEM(packet, jnp.int16),
            pltpu.VMEM((width // LANES, 8, LANES), jnp.float32),
            pltpu.VMEM((space, 8, LANES), jnp.float32),
            pltpu.SemaphoreType.DMA((everyone,)),
            pltpu.SemaphoreType.DMA((everyone,)),
            pltpu.SemaphoreType.DMA((space,)),
            pltpu.SemaphoreType.DMA((space,)),
            pltpu.SemaphoreType.DMA((everyone,)),
            pltpu.SemaphoreType.DMA((everyone,)),
        ],
        compiler_params=pltpu.CompilerParams(collective_id=0, has_side_effects=True),
        name="soot",
    )(density, velocity, kernel, split, target)
    parts = 4
    return pl.pallas_call(
        unpack_kernel,
        grid=(parts,),
        out_shape=jax.ShapeDtypeStruct((planes, block, width), jnp.float32),
        in_specs=[pl.BlockSpec((everyone // parts, planes, ROWS, LANES), lambda i: (i, 0, 0, 0))],
        out_specs=pl.BlockSpec((planes, block, width // parts), lambda i: (0, 0, i)),
        name="unpack",
    )(got)


def on_device(density, velocity, kernel, split, target):
    planes, block, width = density.shape
    sections = kernel.shape[0]
    space, sect = lax.axis_size("space"), lax.axis_size("sect")
    everyone = space * sect
    share = width // everyone
    groups = LANES // share
    tiles = planes * space // groups
    axes = ("space", "sect")
    if 2 * share == LANES and block == 2 * ROWS and space % 2 == 0 and sect % 2 == 0 and planes <= 8:
        return exchanged(density, velocity, kernel, split, target)

    sent = density.reshape(planes, block, everyone, share).transpose(2, 0, 1, 3)
    got = lax.all_to_all(sent, axes, 0, 0, tiled=True)
    got = got.reshape(space, sect, planes, block, share).transpose(1, 3, 0, 2, 4)
    got = got.reshape(sections, groups, tiles, share).transpose(0, 2, 1, 3)
    x = got.reshape(sections, tiles * LANES)

    vsent = velocity.reshape(planes, space, width // space).transpose(1, 0, 2)
    vgot = lax.all_to_all(vsent, "space", 0, 0, tiled=True).reshape(planes * space, width // space)
    v = lax.dynamic_slice_in_dim(vgot, lax.axis_index("sect") * share, share, 1)
    v = v.reshape(groups, tiles, share).transpose(1, 0, 2).reshape(1, tiles * LANES)

    y = compute(x, v, kernel, split, target, share)

    y = y.reshape(sections, tiles, groups, share).transpose(0, 2, 1, 3)
    y = y.reshape(sect, block, space, planes, share).transpose(2, 0, 3, 1, 4)
    y = y.reshape(everyone, planes, block, share)
    back = lax.all_to_all(y, axes, 0, 0, tiled=True)
    return back.transpose(1, 2, 0, 3).reshape(planes, block, width)


def solution(mesh):
    def run(*arrays):
        placed = (P("space", "sect", None), P("space", None), P(), P(), P())
        return jax.shard_map(
            on_device, mesh=mesh, in_specs=placed, out_specs=P("space", "sect", None), check_vma=False
        )(*arrays)

    def traced(*arrays):
        with jax.sharding.use_abstract_mesh(mesh.abstract_mesh):
            return run(*arrays)

    return traced
```
